32 devices in a mesh: gx: 4 (over z), gy: 2 (over y), gz: 4 (over x, core).
Axes of the slice: x: 2, y: 2, z: 4, core: 2. Of those that a mesh axis runs over, the one named last changes fastest.
Arguments:
- strain: float32 [2, 4, 64, 32, 512], P(None, None, 'gx', 'gy', 'gz'), may hold values from -6 to 6
- cell_shell_index: int32 [64, 32, 512], P('gx', 'gy', 'gz'), may hold values from 0 to 255
- onset_step: int32 [256], replicated, may hold values from 0 to 1
Outputs:
- psi_four: float32 [2, 4, 64, 32, 512], P(None, None, 'gx', 'gy', 'gz')
- energy: float32 [4, 4, 256], P('gx', None, ('gy', 'gz'))
The draws below stay inside these ranges and needn't reach their ends.
All inputs are finite; a program needn't handle non-finite values.
Results may differ from the reference program's by a relative error of at most 0.00007.
Values sent between devices are 32-bit elements; how exact they have to be, the bound alone decides.
No kernel may reach another device: no remote copies, remote signals or barrier semaphores. Data moves between devices by JAX's collectives and lax.ppermute only.
A program may use at most 64 MiB of HBM per device.

```python
import jax
import jax.numpy as jnp
from jax import lax

CX = 16
NT = 4
SHELLS = 256
NX = 64
NY = 32
NZ = 512
N_GX = 4


def set_ends(values, stream_key, smallest, largest):
    index_at = [jax.random.randint(jax.random.fold_in(stream_key, axis), (), 0, length) for axis, length in enumerate(values.shape)]
    main_axis = values.shape.index(max(values.shape))
    beside = index_at[:main_axis] + [(index_at[main_axis] + 1) % values.shape[main_axis]] + index_at[main_axis + 1:]
    return values.at[tuple(index_at)].set(smallest).at[tuple(beside)].set(largest)


def block_levels(own_key, dims, pieces, least, high):
    loudness, own = 1.0, jax.random.fold_in(own_key, 6)
    for position, shards_of in pieces:
        heights = jnp.exp(jax.random.uniform(jax.random.fold_in(own, position), (shards_of,), jnp.float32, least / len(pieces), high / len(pieces)))
        loudness = loudness * jnp.repeat(heights, dims[position] // shards_of).reshape([-1 if axis == position else 1 for axis in range(len(dims))])
    return loudness


def centred(rng, extent, spread, limit, split=(), held_as=jnp.bfloat16):
    array = jax.random.normal(rng, extent, jnp.float32) * spread
    if len(split) > 0:
        array = block_levels(rng, extent, split, -0.22, 0.18) * array
    return jnp.clip(array, min=-limit, max=limit).astype(held_as)


def setup_inputs(seed: int = 0) -> dict:
    keys = jax.random.split(jax.random.key(seed), 4)
    strain = centred(keys[0], (2, NT, NX, NY, NZ), 1.0, 6.0, ((2, 4), (3, 2), (4, 4)), jnp.float32)
    cell_shell_index = set_ends(jax.random.randint(keys[1], (NX, NY, NZ), 0, SHELLS), jax.random.fold_in(keys[1], 1), 0, SHELLS - 1).astype(jnp.int32)
    onset_step = set_ends(jax.random.randint(keys[2], (SHELLS,), 0, NT // 2), jax.random.fold_in(keys[2], 1), 0, (NT // 2) - 1).astype(jnp.int32)
    return dict(strain=strain, cell_shell_index=cell_shell_index, onset_step=onset_step)


first_coef = ((-2, 1.0), (-1, -8.0), (1, 8.0), (2, -1.0))
second_coef = ((-2, -1.0), (-1, 16.0), (0, -30.0), (1, 16.0), (2, -1.0))


def take_shifted(padded, off_x, off_y, off_z):
    len_x = padded.shape[2] - 4
    len_y = padded.shape[3] - 4
    len_z = padded.shape[4] - 4
    return padded[:, :, 2 + off_x:2 + off_x + len_x, 2 + off_y:2 + off_y + len_y, 2 + off_z:2 + off_z + len_z]


def reference(strain, cell_shell_index, onset_step):
    padded = jnp.pad(strain, ((0, 0), (0, 0), (2, 2), (2, 2), (2, 2)))
    second_x = sum(w * take_shifted(padded, k, 0, 0) for k, w in second_coef) / 12.0
    second_y = sum(w * take_shifted(padded, 0, k, 0) for k, w in second_coef) / 12.0
    second_z = sum(w * take_shifted(padded, 0, 0, k) for k, w in second_coef) / 12.0
    mixed_yz = sum(wa * wb * take_shifted(padded, 0, ka, kb) for ka, wa in first_coef for kb, wb in first_coef) / 144.0
    combo = second_x + second_y - second_z
    real_part = 0.5 * combo[0] - mixed_yz[1]
    imag_part = -0.5 * combo[1] - mixed_yz[0]
    psi_four = jnp.stack([real_part, imag_part])
    bondi_news = jnp.cumsum(psi_four, axis=1) * 0.25
    position_along_x = (jnp.arange(NX, dtype=jnp.float32) + 0.5) / NX - 0.5
    position_along_y = (jnp.arange(NY, dtype=jnp.float32) + 0.5) / NY - 0.5
    position_along_z = (jnp.arange(NZ, dtype=jnp.float32) + 0.5) / NZ - 0.5
    radius_squared = position_along_x[:, None, None] ** 2 + position_along_y[None, :, None] ** 2 + position_along_z[None, None, :] ** 2 + 0.05
    energy_flux = radius_squared[None] * (bondi_news[0] ** 2 + bondi_news[1] ** 2)
    flux_slabs = energy_flux.reshape(NT, N_GX, CX * NY * NZ)
    id_slabs = cell_shell_index.reshape(N_GX, CX * NY * NZ)

    def per_slab(slab):
        data = lax.dynamic_index_in_dim(flux_slabs, slab, 1, keepdims=False)
        ids = lax.dynamic_index_in_dim(id_slabs, slab, 0, keepdims=False)
        return jax.ops.segment_sum(data.T, ids, num_segments=SHELLS).T

    binned = lax.map(per_slab, jnp.arange(N_GX, dtype=jnp.int32))
    live = (jnp.arange(NT, dtype=jnp.int32)[:, None] >= onset_step[None, :]).astype(jnp.float32)
    binned = binned * live[None]
    scale = 0.25 * SHELLS / (NX * NY * NZ)
    energy = jnp.cumsum(jnp.cumsum(binned, axis=1), axis=0) * scale
    return psi_four, energy
```

```python
import jax
import jax.numpy as jnp
from jax import lax
from jax.experimental import pallas as pl
from jax.experimental.pallas import tpu as pltpu
from jax.sharding import PartitionSpec as P


LANES = 128
F32 = jnp.float32
VMEM = pl.BlockSpec(memory_space=pltpu.VMEM)


def lane_iota(rows):
    return lax.broadcasted_iota(jnp.int32, (rows, LANES), 1)


def row_iota(rows):
    return lax.broadcasted_iota(jnp.int32, (rows, LANES), 0)


def shift_lanes(v, offset, lane):
    moved = pltpu.roll(v, (-offset) % LANES, 1)
    inside = lane < LANES - offset if offset > 0 else lane >= -offset
    return jnp.where(inside, moved, 0.0)


def pack_kernel(two_y, s_ref, *outs):
    comps, steps, cx, cy, cz = s_ref.shape
    x_tail, x_head, z_edges = outs[:3]
    y_sends = outs[3:]
    for c in range(comps):
        for t in range(steps):
            x_tail[c, t] = s_ref[c, t, cx - 2 :]
            x_head[c, t] = s_ref[c, t, :2]
    rows = s_ref.reshape(comps * steps * cx * cy, cz)
    count = comps * steps * cx
    if two_y:
        start = jnp.where(lax.axis_index("gy") == 0, cy - 2, 0)
        starts = (start,)
    else:
        starts = (cy - 2, 0)
    for send, start in zip(y_sends, starts):
        for r in range(2):
            send[r] = rows[pl.ds(start + r, count, stride=cy), :]
    lane = lane_iota(cy)
    group = lane // 4
    per = LANES // 4
    for col in range(count // per):
        packed = jnp.zeros((cy, LANES), F32)
        for i in range(per):
            k = col * per + i
            block = s_ref[k // (steps * cx), (k // cx) % steps, k % cx]
            packed = jnp.where(group == i, pltpu.roll(block, (2 + 4 * i) % LANES, 1), packed)
        z_edges[col] = packed


def local_kernel(s_ref, psi_ref, pad_ref):
    comps, steps, cx, cy, cz = s_ref.shape
    lane = lane_iota(cy)
    pad_ref[...] = jnp.zeros_like(pad_ref)

    def plane(x, carry):
        for t in range(steps):
            lap, mix = [], []
            for c in range(comps):
                s = s_ref[c, t, x]
                m2, m1, p1, p2 = (shift_lanes(s, k, lane) for k in (-2, -1, 1, 2))
                near_z, far_z = m1 + p1, m2 + p2
                first_z = 8.0 * (p1 - m1) - (p2 - m2)
                pad_ref[t, c, 0, 8 : 8 + cy] = s
                pad_ref[t, c, 1, 8 : 8 + cy] = first_z
                at = lambda q, k: pad_ref[t, c, q, 8 + k : 8 + k + cy]
                near, far = at(0, -1) + at(0, 1), at(0, -2) + at(0, 2)
                for k in (1, 2):
                    low = s_ref[c, t, jnp.maximum(x - k, 0)] * (x >= k).astype(F32)
                    high = s_ref[c, t, jnp.minimum(x + k, cx - 1)] * (x < cx - k).astype(F32)
                    if k == 1:
                        near = near + (low + high)
                    else:
                        far = far + (low + high)
                lap.append(16.0 * (near - near_z) - (far - far_z) - 30.0 * s)
                mix.append(8.0 * (at(1, 1) - at(1, -1)) - (at(1, 2) - at(1, -2)))
            psi_ref[0, t, x] = (0.5 / 12.0) * lap[0] - (1.0 / 144.0) * mix[1]
            psi_ref[1, t, x] = (-0.5 / 12.0) * lap[1] - (1.0 / 144.0) * mix[0]
        return carry

    lax.fori_loop(0, cx, plane, 0)


def finish_kernel(
    sizes,
    local_ref, shell_ref, onset_ref,
    x_low, x_high, y_low, y_high, z_low, z_high, ll, lh, hl, hh,
    psi_ref, part_ref,
    x_fix, y_fix, z_ext, z_dz, z_fix, flux_ref, left_ref, right_ref,
):
    comps, steps, cx, cy, cz = local_ref.shape
    n_x, n_y, n_z = sizes
    gx, gy, gz = (lax.axis_index(a) for a in ("gx", "gy", "gz"))
    half, twelfth = 0.5 / 12.0, 1.0 / 144.0
    sign = (half, -half)
    has = lambda ok: ok.astype(F32)
    has_x = (has(gx > 0), has(gx < n_x - 1))
    has_y = (has(gy > 0), has(gy < n_y - 1))
    has_z = (has(gz > 0), has(gz < n_z - 1))
    count = comps * steps * cx

    for c in range(comps):
        low, high = sign[c] * has_x[0], sign[c] * has_x[1]
        for t in range(steps):
            a, b = x_low[c, t, 0], x_low[c, t, 1]
            x_fix[0, c, t] = low * (16.0 * b - a)
            x_fix[1, c, t] = -low * b
            a, b = x_high[c, t, 0], x_high[c, t, 1]
            x_fix[2, c, t] = -high * a
            x_fix[3, c, t] = high * (16.0 * a - b)

    y_fix[...] = jnp.zeros_like(y_fix)
    own = count // comps
    lane8 = lane_iota(8)

    def y_rows(side, src):
        for start in range(0, own, 8):
            vals = []
            for c in range(comps):
                pair = []
                for r in range(2):
                    h = src[r, c * own + start : c * own + start + 8]
                    m2, m1, p1, p2 = (shift_lanes(h, k, lane8) for k in (-2, -1, 1, 2))
                    pair.append((h, 8.0 * (p1 - m1) - (p2 - m2)))
                (h0, d0), (h1, d1) = pair
                if side == 0:
                    vals.append(((16.0 * h1 - h0, d0 - 8.0 * d1), (-h1, d1)))
                else:
                    vals.append(((-h0, -d0), (16.0 * h0 - h1, 8.0 * d0 - d1)))
            for c in range(comps):
                for r in range(2):
                    fix = sign[c] * vals[c][r][0] - twelfth * vals[1 - c][r][1]
                    base = (side * count + c * own + start) * 8 + (0 if side == 0 else 6) + r
                    y_fix[pl.ds(base, 8, stride=8), :] = fix

    @pl.when(gy > 0)
    def _():
        y_rows(0, y_low)

    @pl.when(gy < n_y - 1)
    def _():
        y_rows(1, y_high)

    cols = count * 4 // LANES
    z_ext[...] = jnp.zeros_like(z_ext)
    spot = lane_iota(cy) % 4
    spot32 = lane_iota(cy + 16) % 4
    for col in range(cols):
        z_ext[col, 8 : 8 + cy] = jnp.where(spot < 2, z_low[col] * has_z[0], z_high[col] * has_z[1])
        z_ext[col, 6:8] = has_y[0] * jnp.where(
            spot[:2] < 2, ll[col, cy - 2 :] * has_z[0], lh[col, cy - 2 :] * has_z[1]
        )
        z_ext[col, 8 + cy : 10 + cy] = has_y[1] * jnp.where(
            spot[:2] < 2, hl[col, :2] * has_z[0], hh[col, :2] * has_z[1]
        )
    seconds = []
    for col in range(cols):
        v = z_ext[col]
        r2, l2 = pltpu.roll(v, 2, 1), pltpu.roll(v, LANES - 2, 1)
        r1, l1 = pltpu.roll(v, 1, 1), pltpu.roll(v, LANES - 1, 1)
        far = jnp.where(spot32 >= 2, r2, l2)
        near = jnp.where(spot32 == 2, r1, jnp.where(spot32 == 1, l1, 0.0))
        signed = jnp.where(spot32 >= 2, far - 8.0 * near, 8.0 * near - far)
        z_dz[col] = signed
        seconds.append((16.0 * near - far)[8 : 8 + cy])
    for col in range(cols):
        c = col // (cols // comps)
        other = col + cols // comps if c == 0 else col - cols // comps
        at = lambda k: z_dz[other, 8 + k : 8 + k + cy]
        mix = 8.0 * (at(1) - at(-1)) - (at(2) - at(-2))
        z_fix[col] = -sign[c] * seconds[col] - twelfth * mix

    lane = lane_iota(cy)
    edge = (lane < 2) | (lane >= LANES - 2)
    total_x, total_y, total_z = n_x * cx, n_y * cy, n_z * cz
    at_y = (row_iota(cy) + gy * cy).astype(F32)
    at_z = (lane + gz * cz).astype(F32)
    uy = (at_y + 0.5) / total_y - 0.5
    uz = (at_z + 0.5) / total_z - 0.5
    yz = uy * uy + uz * uz
    low_count = right_ref.shape[0]
    high_count = onset_ref.shape[0]
    high_iota = row_iota(high_count)
    low_iota = row_iota(low_count)
    per = LANES // 4

    def plane(x, total):
        for c in range(comps):
            for t in range(steps):
                k = t * cx
                col = (c * own + k) // per
                fix = pltpu.roll(z_fix[col], (LANES - 2 - 4 * (k % per + x)) % LANES, 1)
                v = local_ref[c, t, x] + jnp.where(edge, fix, 0.0)
                row = (c * own + k + x) * 8
                psi_ref[c, t, x, :8] = v[:8] + y_fix[pl.ds(row, 8), :]
                if cy > 16:
                    psi_ref[c, t, x, 8 : cy - 8] = v[8 : cy - 8]
                psi_ref[c, t, x, cy - 8 :] = v[cy - 8 :] + y_fix[pl.ds(row + count * 8, 8), :]

        @pl.when((x < 2) | (x >= cx - 2))
        def _():
            slot = jnp.where(x < 2, x, x - (cx - 4))
            for c in range(comps):
                for t in range(steps):
                    psi_ref[c, t, x] += x_fix[slot, c, t]

        ux = ((gx * cx + x).astype(F32) + 0.5) / total_x - 0.5
        weight = 0.0625 * (ux * ux + yz + 0.05)
        real = jnp.zeros((cy, LANES), F32)
        imag = jnp.zeros((cy, LANES), F32)
        for t in range(steps):
            real = real + psi_ref[0, t, x]
            imag = imag + psi_ref[1, t, x]
            flux = weight * (real * real + imag * imag)
            head = flux.astype(jnp.bfloat16).astype(F32)
            flux_ref[0, t] = head
            flux_ref[1, t] = flux - head
        for y in range(cy):
            shell = jnp.broadcast_to(shell_ref[x, pl.ds(y, 1), :], (low_count, LANES))
            high = shell[:high_count] // low_count == high_iota
            low = jnp.where(shell % low_count == low_iota, 1.0, 0.0)
            right_ref[:, y * LANES : (y + 1) * LANES] = low.astype(jnp.bfloat16)
            pieces = []
            for part in range(2):
                for t in range(steps):
                    f = jnp.broadcast_to(flux_ref[part, t, pl.ds(y, 1), :], (high_count, LANES))
                    pieces.append(jnp.where(high, f, 0.0))
            left_ref[:, y * LANES : (y + 1) * LANES] = jnp.concatenate(pieces).astype(jnp.bfloat16)
        return total + lax.dot_general(
            left_ref[...], right_ref[...], (((1,), (1,)), ((), ())), preferred_element_type=F32
        )

    rows = 2 * steps * high_count
    total = lax.fori_loop(0, cx, plane, jnp.zeros((rows, low_count), F32))
    scale = 0.25 * (high_count * low_count) / (total_x * total_y * total_z)
    onset = onset_ref[...]
    running = jnp.zeros((high_count, low_count), F32)
    for t in range(steps):
        a = total[t * high_count : (t + 1) * high_count]
        b = total[(steps + t) * high_count : (steps + t + 1) * high_count]
        running = running + jnp.where(t >= onset, a + b, 0.0)
        for g in range(n_x):
            part_ref[g, :, t] = jnp.where(gx <= g, running * scale, 0.0)


def call(kernel, outs, scratch=(), flops=0):
    return pl.pallas_call(
        kernel,
        out_shape=tuple(jax.ShapeDtypeStruct(s, F32) for s in outs),
        scratch_shapes=scratch,
        cost_estimate=pl.CostEstimate(flops=flops, transcendentals=0, bytes_accessed=2**20),
    )


def ring(value, axis, shift):
    count = lax.axis_size(axis)
    return lax.ppermute(value, axis, [(i, (i + shift) % count) for i in range(count)])


def corner(value, n_y, n_z, dy, dz):
    pairs = [
        (a * n_z + b, ((a + dy) % n_y) * n_z + (b + dz) % n_z) for a in range(n_y) for b in range(n_z)
    ]
    return lax.ppermute(value, ("gy", "gz"), pairs)


def body(strain, cell_shell_index, onset_step):
    comps, steps, cx, cy, cz = strain.shape
    sizes = n_x, n_y, n_z = tuple(lax.axis_size(a) for a in ("gx", "gy", "gz"))
    shells = onset_step.shape[0]
    low_count = 32
    high_count = shells // low_count
    count = comps * steps * cx
    two_y = n_y == 2
    x_msg = (comps, steps, 2, cy, cz)
    y_msg = (2, count, cz)
    z_msg = (count * 4 // LANES, cy, LANES)
    sent = call(
        lambda *refs: pack_kernel(two_y, *refs),
        (x_msg, x_msg, z_msg) + (y_msg,) * (1 if two_y else 2),
    )(strain)
    x_tail, x_head, z_edges = sent[:3]
    x_low, x_high = ring(x_tail, "gx", 1), ring(x_head, "gx", -1)
    if two_y:
        y_low = y_high = ring(sent[3], "gy", 1)
    else:
        y_low, y_high = ring(sent[3], "gy", 1), ring(sent[4], "gy", -1)
    z_low, z_high = ring(z_edges, "gz", 1), ring(z_edges, "gz", -1)
    ll, lh = corner(z_edges, n_y, n_z, 1, 1), corner(z_edges, n_y, n_z, 1, -1)
    if two_y:
        hl, hh = ll, lh
    else:
        hl, hh = corner(z_edges, n_y, n_z, -1, 1), corner(z_edges, n_y, n_z, -1, -1)

    local = call(
        local_kernel,
        (strain.shape,),
        [pltpu.VMEM((steps, comps, 2, cy + 16, cz), F32)],
        flops=10**8,
    )(strain)[0]

    own_rows = 2 * count * 8
    psi, part = call(
        lambda *refs: finish_kernel(sizes, *refs),
        (strain.shape, (n_x, high_count, steps, low_count)),
        [
            pltpu.VMEM((4, comps, steps, cy, cz), F32),
            pltpu.VMEM((own_rows, cz), F32),
            pltpu.VMEM((z_msg[0], cy + 16, LANES), F32),
            pltpu.VMEM((z_msg[0], cy + 16, LANES), F32),
            pltpu.VMEM(z_msg, F32),
            pltpu.VMEM((2, steps, cy, cz), F32),
            pltpu.VMEM((2 * steps * high_count, cy * cz), jnp.bfloat16),
            pltpu.VMEM((low_count, cy * cz), jnp.bfloat16),
        ],
        flops=10**8,
    )(
        local, cell_shell_index, onset_step.reshape(high_count, low_count),
        x_low, x_high, y_low, y_high, z_low, z_high, ll, lh, hl, hh,
    )

    shards = n_y * n_z
    per = shells // shards
    part = part.transpose(0, 2, 1, 3).reshape(n_x, steps, shards, per).transpose(0, 2, 1, 3)
    part = part.reshape(n_x * shards, steps, per)
    got = lax.all_to_all(part, ("gx", "gy", "gz"), 0, 0, tiled=True)
    return psi, jnp.sum(got, axis=0)[None]


def solution(mesh):
    placed = (P(None, None, "gx", "gy", "gz"), P("gx", "gy", "gz"), P())
    return jax.shard_map(
        body,
        mesh=mesh,
        in_specs=placed,
        out_specs=(P(None, None, "gx", "gy", "gz"), P("gx", None, ("gy", "gz"))),
        check_vma=False,
    )
```

```python
import jax
import jax.numpy as jnp
from jax import lax
from jax.experimental import pallas as pl
from jax.experimental.pallas import tpu as pltpu
from jax.sharding import PartitionSpec as P


LANES = 128
F32 = jnp.float32
VMEM_LIMIT = 24 * 2**20


def lane_iota(rows):
    return lax.broadcasted_iota(jnp.int32, (rows, LANES), 1)


def row_iota(rows):
    return lax.broadcasted_iota(jnp.int32, (rows, LANES), 0)


def shift_lanes(v, offset, lane):
    moved = pltpu.roll(v, (-offset) % LANES, 1)
    inside = lane < LANES - offset if offset > 0 else lane >= -offset
    return jnp.where(inside, moved, 0.0)


def pack_kernel(two_y, s_ref, *outs):
    comps, steps, cx, cy, cz = s_ref.shape
    x_tail, x_head, z_edges = outs[:3]
    y_sends = outs[3:]
    for c in range(comps):
        for t in range(steps):
            x_tail[c, t] = s_ref[c, t, cx - 2 :]
            x_head[c, t] = s_ref[c, t, :2]
    rows = s_ref.reshape(comps * steps * cx * cy, cz)
    count = comps * steps * cx
    if two_y:
        start = jnp.where(lax.axis_index("gy") == 0, cy - 2, 0)
        starts = (start,)
    else:
        starts = (cy - 2, 0)
    for send, start in zip(y_sends, starts):
        for r in range(2):
            send[r] = rows[pl.ds(start + r, count, stride=cy), :]
    lane = lane_iota(cy)
    group = lane // 4
    per = LANES // 4
    for col in range(count // per):
        packed = jnp.zeros((cy, LANES), F32)
        for i in range(per):
            k = col * per + i
            block = s_ref[k // (steps * cx), (k // cx) % steps, k % cx]
            packed = jnp.where(group == i, pltpu.roll(block, (2 + 4 * i) % LANES, 1), packed)
        z_edges[col] = packed


def local_kernel(s_ref, psi_ref, pad_ref):
    comps, steps, cx, cy, cz = s_ref.shape
    lane = lane_iota(cy)
    pad_ref[...] = jnp.zeros_like(pad_ref)

    def plane(x, carry):
        for t in range(steps):
            lap, mix = [], []
            for c in range(comps):
                s = s_ref[c, t, x]
                m2, m1, p1, p2 = (shift_lanes(s, k, lane) for k in (-2, -1, 1, 2))
                near_z, far_z = m1 + p1, m2 + p2
                first_z = 8.0 * (p1 - m1) - (p2 - m2)
                pad_ref[t, c, 0, 8 : 8 + cy] = s
                pad_ref[t, c, 1, 8 : 8 + cy] = first_z
                at = lambda q, k: pad_ref[t, c, q, 8 + k : 8 + k + cy]
                near, far = at(0, -1) + at(0, 1), at(0, -2) + at(0, 2)
                for k in (1, 2):
                    low = s_ref[c, t, jnp.maximum(x - k, 0)] * (x >= k).astype(F32)
                    high = s_ref[c, t, jnp.minimum(x + k, cx - 1)] * (x < cx - k).astype(F32)
                    if k == 1:
                        near = near + (low + high)
                    else:
                        far = far + (low + high)
                lap.append(16.0 * (near - near_z) - (far - far_z) - 30.0 * s)
                mix.append(8.0 * (at(1, 1) - at(1, -1)) - (at(1, 2) - at(1, -2)))
            psi_ref[0, t, x] = (0.5 / 12.0) * lap[0] - (1.0 / 144.0) * mix[1]
            psi_ref[1, t, x] = (-0.5 / 12.0) * lap[1] - (1.0 / 144.0) * mix[0]
        return carry

    lax.fori_loop(0, cx, plane, 0)


def finish_kernel(
    sizes,
    local_ref, shell_ref, onset_ref,
    x_low, x_high, y_low, y_high, z_low, z_high, ll, lh, hl, hh,
    psi_ref, part_ref,
    x_fix, y_fix, z_ext, z_dz, z_fix, flux_ref, left_ref, right_ref,
):
    comps, steps, cx, cy, cz = local_ref.shape
    n_x, n_y, n_z = sizes
    gx, gy, gz = (lax.axis_index(a) for a in ("gx", "gy", "gz"))
    half, twelfth = 0.5 / 12.0, 1.0 / 144.0
    sign = (half, -half)
    has = lambda ok: ok.astype(F32)
    has_x = (has(gx > 0), has(gx < n_x - 1))
    has_y = (has(gy > 0), has(gy < n_y - 1))
    has_z = (has(gz > 0), has(gz < n_z - 1))
    count = comps * steps * cx

    for c in range(comps):
        low, high = sign[c] * has_x[0], sign[c] * has_x[1]
        for t in range(steps):
            a, b = x_low[c, t, 0], x_low[c, t, 1]
            x_fix[0, c, t] = low * (16.0 * b - a)
            x_fix[1, c, t] = -low * b
            a, b = x_high[c, t, 0], x_high[c, t, 1]
            x_fix[2, c, t] = -high * a
            x_fix[3, c, t] = high * (16.0 * a - b)

    y_fix[...] = jnp.zeros_like(y_fix)
    own = count // comps
    lane8 = lane_iota(8)

    def y_rows(side, src):
        for start in range(0, own, 8):
            vals = []
            for c in range(comps):
                pair = []
                for r in range(2):
                    h = src[r, c * own + start : c * own + start + 8]
                    m2, m1, p1, p2 = (shift_lanes(h, k, lane8) for k in (-2, -1, 1, 2))
                    pair.append((h, 8.0 * (p1 - m1) - (p2 - m2)))
                (h0, d0), (h1, d1) = pair
                if side == 0:
                    vals.append(((16.0 * h1 - h0, d0 - 8.0 * d1), (-h1, d1)))
                else:
                    vals.append(((-h0, -d0), (16.0 * h0 - h1, 8.0 * d0 - d1)))
            for c in range(comps):
                for r in range(2):
                    fix = sign[c] * vals[c][r][0] - twelfth * vals[1 - c][r][1]
                    base = (side * count + c * own + start) * 8 + (0 if side == 0 else 6) + r
                    y_fix[pl.ds(base, 8, stride=8), :] = fix

    @pl.when(gy > 0)
    def _():
        y_rows(0, y_low)

    @pl.when(gy < n_y - 1)
    def _():
        y_rows(1, y_high)

    cols = count * 4 // LANES
    z_ext[...] = jnp.zeros_like(z_ext)
    spot = lane_iota(cy) % 4
    spot32 = lane_iota(cy + 16) % 4
    for col in range(cols):
        z_ext[col, 8 : 8 + cy] = jnp.where(spot < 2, z_low[col] * has_z[0], z_high[col] * has_z[1])
        z_ext[col, 6:8] = has_y[0] * jnp.where(
            spot[:2] < 2, ll[col, cy - 2 :] * has_z[0], lh[col, cy - 2 :] * has_z[1]
        )
        z_ext[col, 8 + cy : 10 + cy] = has_y[1] * jnp.where(
            spot[:2] < 2, hl[col, :2] * has_z[0], hh[col, :2] * has_z[1]
        )
    seconds = []
    for col in range(cols):
        v = z_ext[col]
        r2, l2 = pltpu.roll(v, 2, 1), pltpu.roll(v, LANES - 2, 1)
        r1, l1 = pltpu.roll(v, 1, 1), pltpu.roll(v, LANES - 1, 1)
        far = jnp.where(spot32 >= 2, r2, l2)
        near = jnp.where(spot32 == 2, r1, jnp.where(spot32 == 1, l1, 0.0))
        signed = jnp.where(spot32 >= 2, far - 8.0 * near, 8.0 * near - far)
        z_dz[col] = signed
        seconds.append((16.0 * near - far)[8 : 8 + cy])
    for col in range(cols):
        c = col // (cols // comps)
        other = col + cols // comps if c == 0 else col - cols // comps
        at = lambda k: z_dz[other, 8 + k : 8 + k + cy]
        mix = 8.0 * (at(1) - at(-1)) - (at(2) - at(-2))
        z_fix[col] = -sign[c] * seconds[col] - twelfth * mix

    lane = lane_iota(cy)
    edge = (lane < 2) | (lane >= LANES - 2)
    total_x, total_y, total_z = n_x * cx, n_y * cy, n_z * cz
    at_y = (row_iota(cy) + gy * cy).astype(F32)
    at_z = (lane + gz * cz).astype(F32)
    uy = (at_y + 0.5) / total_y - 0.5
    uz = (at_z + 0.5) / total_z - 0.5
    yz = uy * uy + uz * uz
    low_count = right_ref.shape[0]
    high_count = left_ref.shape[0] // (2 * steps)
    high_iota = row_iota(high_count)
    low_iota = row_iota(low_count)
    per = LANES // 4

    def plane(x, total):
        for c in range(comps):
            for t in range(steps):
                k = t * cx
                col = (c * own + k) // per
                fix = pltpu.roll(z_fix[col], (LANES - 2 - 4 * (k % per + x)) % LANES, 1)
                v = local_ref[c, t, x] + jnp.where(edge, fix, 0.0)
                row = (c * own + k + x) * 8
                psi_ref[c, t, x, :8] = v[:8] + y_fix[pl.ds(row, 8), :]
                if cy > 16:
                    psi_ref[c, t, x, 8 : cy - 8] = v[8 : cy - 8]
                psi_ref[c, t, x, cy - 8 :] = v[cy - 8 :] + y_fix[pl.ds(row + count * 8, 8), :]

        @pl.when((x < 2) | (x >= cx - 2))
        def _():
            slot = jnp.where(x < 2, x, x - (cx - 4))
            for c in range(comps):
                for t in range(steps):
                    psi_ref[c, t, x] += x_fix[slot, c, t]

        ux = ((gx * cx + x).astype(F32) + 0.5) / total_x - 0.5
        weight = 0.0625 * (ux * ux + yz + 0.05)
        real = jnp.zeros((cy, LANES), F32)
        imag = jnp.zeros((cy, LANES), F32)
        for t in range(steps):
            real = real + psi_ref[0, t, x]
            imag = imag + psi_ref[1, t, x]
            flux = weight * (real * real + imag * imag)
            head = flux.astype(jnp.bfloat16).astype(F32)
            flux_ref[0, t] = head
            flux_ref[1, t] = flux - head
        for y in range(cy):
            shell = jnp.broadcast_to(shell_ref[x, pl.ds(y, 1), :], (low_count, LANES))
            high = shell[:high_count] // low_count == high_iota
            low = jnp.where(shell % low_count == low_iota, 1.0, 0.0)
            right_ref[:, y * LANES : (y + 1) * LANES] = low.astype(jnp.bfloat16)
            pieces = []
            for part in range(2):
                for t in range(steps):
                    f = jnp.broadcast_to(flux_ref[part, t, pl.ds(y, 1), :], (high_count, LANES))
                    pieces.append(jnp.where(high, f, 0.0))
            left_ref[:, y * LANES : (y + 1) * LANES] = jnp.concatenate(pieces).astype(jnp.bfloat16)
        return total + lax.dot_general(
            left_ref[...], right_ref[...], (((1,), (1,)), ((), ())), preferred_element_type=F32
        )

    rows = 2 * steps * high_count
    total = lax.fori_loop(0, cx, plane, jnp.zeros((rows, low_count), F32))
    scale = 0.25 * (high_count * low_count) / (total_x * total_y * total_z)
    onset = onset_table(onset_ref, high_count, low_count)
    running = jnp.zeros((high_count, low_count), F32)
    sums = []
    for t in range(steps):
        a = total[t * high_count : (t + 1) * high_count]
        b = total[(steps + t) * high_count : (steps + t + 1) * high_count]
        running = running + jnp.where(t >= onset, a + b, 0.0)
        sums.append(running * scale)
    if len(part_ref.shape) == 4:
        for g in range(n_x):
            for t in range(steps):
                part_ref[g, :, t] = jnp.where(gx <= g, sums[t], 0.0)
    else:
        joined = jnp.concatenate(sums, axis=1)
        for g in range(n_x):
            part_ref[g] = jnp.where(gx <= g, joined, 0.0)


def onset_table(onset_ref, high_count, low_count):
    fold = LANES // low_count
    row = row_iota(high_count)
    table = jnp.zeros((high_count, LANES), jnp.int32)
    for h in range(high_count):
        line = jnp.broadcast_to(onset_ref[h // fold : h // fold + 1], (high_count, LANES))
        line = pltpu.roll(line, (LANES - (h % fold) * low_count) % LANES, 1)
        table = jnp.where(row == h, line, table)
    return table[:, :low_count]


def sum_kernel(got_ref, out_ref):
    steps, per = out_ref.shape[1:]
    total = jnp.sum(got_ref[...], axis=0, keepdims=True)
    for t in range(steps):
        out_ref[0, t : t + 1, :] = total[:, t * per : (t + 1) * per]


def call(kernel, outs, scratch=(), flops=0):
    return pl.pallas_call(
        kernel,
        out_shape=tuple(jax.ShapeDtypeStruct(s, F32) for s in outs),
        scratch_shapes=scratch,
        compiler_params=pltpu.CompilerParams(vmem_limit_bytes=VMEM_LIMIT),
        cost_estimate=pl.CostEstimate(flops=flops, transcendentals=0, bytes_accessed=2**20),
    )


def ring(value, axis, shift):
    count = lax.axis_size(axis)
    return lax.ppermute(value, axis, [(i, (i + shift) % count) for i in range(count)])


def corner(value, n_y, n_z, dy, dz):
    pairs = [
        (a * n_z + b, ((a + dy) % n_y) * n_z + (b + dz) % n_z) for a in range(n_y) for b in range(n_z)
    ]
    return lax.ppermute(value, ("gy", "gz"), pairs)


def body(strain, cell_shell_index, onset_step):
    comps, steps, cx, cy, cz = strain.shape
    sizes = n_x, n_y, n_z = tuple(lax.axis_size(a) for a in ("gx", "gy", "gz"))
    shells = onset_step.shape[0]
    low_count = 32
    high_count = shells // low_count
    count = comps * steps * cx
    two_y = n_y == 2
    x_msg = (comps, steps, 2, cy, cz)
    y_msg = (2, count, cz)
    z_msg = (count * 4 // LANES, cy, LANES)
    sent = call(
        lambda *refs: pack_kernel(two_y, *refs),
        (x_msg, x_msg, z_msg) + (y_msg,) * (1 if two_y else 2),
    )(strain)
    x_tail, x_head, z_edges = sent[:3]
    x_low, x_high = ring(x_tail, "gx", 1), ring(x_head, "gx", -1)
    if two_y:
        y_low = y_high = ring(sent[3], "gy", 1)
    else:
        y_low, y_high = ring(sent[3], "gy", 1), ring(sent[4], "gy", -1)
    z_low, z_high = ring(z_edges, "gz", 1), ring(z_edges, "gz", -1)
    ll, lh = corner(z_edges, n_y, n_z, 1, 1), corner(z_edges, n_y, n_z, 1, -1)
    if two_y:
        hl, hh = ll, lh
    else:
        hl, hh = corner(z_edges, n_y, n_z, -1, 1), corner(z_edges, n_y, n_z, -1, -1)

    local = call(
        local_kernel,
        (strain.shape,),
        [pltpu.VMEM((steps, comps, 2, cy + 16, cz), F32)],
        flops=10**8,
    )(strain)[0]

    shards = n_y * n_z
    per = shells // shards
    direct = per == low_count and steps * per == LANES
    own_rows = 2 * count * 8
    psi, part = call(
        lambda *refs: finish_kernel(sizes, *refs),
        (strain.shape, (n_x, shards, LANES) if direct else (n_x, high_count, steps, low_count)),
        [
            pltpu.VMEM((4, comps, steps, cy, cz), F32),
            pltpu.VMEM((own_rows, cz), F32),
            pltpu.VMEM((z_msg[0], cy + 16, LANES), F32),
            pltpu.VMEM((z_msg[0], cy + 16, LANES), F32),
            pltpu.VMEM(z_msg, F32),
            pltpu.VMEM((2, steps, cy, cz), F32),
            pltpu.VMEM((2 * steps * high_count, cy * cz), jnp.bfloat16),
            pltpu.VMEM((low_count, cy * cz), jnp.bfloat16),
        ],
        flops=10**8,
    )(
        local, cell_shell_index, onset_step.reshape(-1, LANES),
        x_low, x_high, y_low, y_high, z_low, z_high, ll, lh, hl, hh,
    )

    axes = ("gx", "gy", "gz")
    if direct:
        got = lax.all_to_all(part.reshape(n_x * shards, LANES), axes, 0, 0, tiled=True)
        return psi, call(sum_kernel, ((1, steps, per),))(got)[0]
    part = part.transpose(0, 2, 1, 3).reshape(n_x, steps, shards, per).transpose(0, 2, 1, 3)
    got = lax.all_to_all(part.reshape(n_x * shards, steps, per), axes, 0, 0, tiled=True)
    return psi, jnp.sum(got, axis=0)[None]


def solution(mesh):
    placed = (P(None, None, "gx", "gy", "gz"), P("gx", "gy", "gz"), P())
    return jax.shard_map(
        body,
        mesh=mesh,
        in_specs=placed,
        out_specs=(P(None, None, "gx", "gy", "gz"), P("gx", None, ("gy", "gz"))),
        check_vma=False,
    )
```

```python
import jax
import jax.numpy as jnp
from jax import lax
from jax.experimental import pallas as pl
from jax.experimental.pallas import tpu as pltpu
from jax.sharding import PartitionSpec as P


LANES = 128
F32 = jnp.float32
UNROLL = 8
VMEM_LIMIT = 24 * 2**20


def lane_iota(rows):
    return lax.broadcasted_iota(jnp.int32, (rows, LANES), 1)


def row_iota(rows):
    return lax.broadcasted_iota(jnp.int32, (rows, LANES), 0)


def shift_lanes(v, offset, lane):
    moved = pltpu.roll(v, (-offset) % LANES, 1)
    inside = lane < LANES - offset if offset > 0 else lane >= -offset
    return jnp.where(inside, moved, 0.0)


def pack_kernel(two_y, s_ref, *outs):
    comps, steps, cx, cy, cz = s_ref.shape
    x_tail, x_head, z_edges = outs[:3]
    y_sends = outs[3:]
    for c in range(comps):
        for t in range(steps):
            x_tail[c, t] = s_ref[c, t, cx - 2 :]
            x_head[c, t] = s_ref[c, t, :2]
    rows = s_ref.reshape(comps * steps * cx * cy, cz)
    count = comps * steps * cx
    if two_y:
        start = jnp.where(lax.axis_index("gy") == 0, cy - 2, 0)
        starts = (start,)
    else:
        starts = (cy - 2, 0)
    for send, start in zip(y_sends, starts):
        for r in range(2):
            send[r] = rows[pl.ds(start + r, count, stride=cy), :]
    lane = lane_iota(cy)
    group = lane // 4
    per = LANES // 4
    for col in range(count // per):
        packed = jnp.zeros((cy, LANES), F32)
        for i in range(per):
            k = col * per + i
            block = s_ref[k // (steps * cx), (k // cx) % steps, k % cx]
            packed = jnp.where(group == i, pltpu.roll(block, (2 + 4 * i) % LANES, 1), packed)
        z_edges[col] = packed


def local_kernel(low_count, s_ref, onset_ref, table, psi_ref, pad_ref):
    table[...] = onset_table(onset_ref, table.shape[0], low_count)
    comps, steps, cx, cy, cz = s_ref.shape
    lane = lane_iota(cy)
    pad_ref[...] = jnp.zeros_like(pad_ref)

    def plane(x, carry):
        for t in range(steps):
            lap, mix = [], []
            for c in range(comps):
                s = s_ref[c, t, x]
                m2, m1, p1, p2 = (shift_lanes(s, k, lane) for k in (-2, -1, 1, 2))
                near_z, far_z = m1 + p1, m2 + p2
                first_z = 8.0 * (p1 - m1) - (p2 - m2)
                pad_ref[t, c, 0, 8 : 8 + cy] = s
                pad_ref[t, c, 1, 8 : 8 + cy] = first_z
                at = lambda q, k: pad_ref[t, c, q, 8 + k : 8 + k + cy]
                near, far = at(0, -1) + at(0, 1), at(0, -2) + at(0, 2)
                for k in (1, 2):
                    low = s_ref[c, t, jnp.maximum(x - k, 0)] * (x >= k).astype(F32)
                    high = s_ref[c, t, jnp.minimum(x + k, cx - 1)] * (x < cx - k).astype(F32)
                    if k == 1:
                        near = near + (low + high)
                    else:
                        far = far + (low + high)
                lap.append(16.0 * (near - near_z) - (far - far_z) - 30.0 * s)
                mix.append(8.0 * (at(1, 1) - at(1, -1)) - (at(1, 2) - at(1, -2)))
            psi_ref[0, t, x] = (0.5 / 12.0) * lap[0] - (1.0 / 144.0) * mix[1]
            psi_ref[1, t, x] = (-0.5 / 12.0) * lap[1] - (1.0 / 144.0) * mix[0]
        return carry

    lax.fori_loop(0, cx, plane, 0)


def finish_kernel(
    sizes, high_count, low_count,
    local_ref, shell_ref, onset_ref,
    x_low, x_high, y_low, y_high, z_low, z_high, ll, lh, hl, hh,
    psi_out, part_ref,
    psi_ref, sent, x_fix, y_fix, z_ext, z_dz, z_fix, flux_ref,
):
    comps, steps, cx, cy, cz = local_ref.shape
    n_x, n_y, n_z = sizes
    gx, gy, gz = (lax.axis_index(a) for a in ("gx", "gy", "gz"))
    half, twelfth = 0.5 / 12.0, 1.0 / 144.0
    sign = (half, -half)
    has = lambda ok: ok.astype(F32)
    has_x = (has(gx > 0), has(gx < n_x - 1))
    has_y = (has(gy > 0), has(gy < n_y - 1))
    has_z = (has(gz > 0), has(gz < n_z - 1))
    count = comps * steps * cx

    for c in range(comps):
        low, high = sign[c] * has_x[0], sign[c] * has_x[1]
        for t in range(steps):
            a, b = x_low[c, t, 0], x_low[c, t, 1]
            x_fix[0, c, t] = low * (16.0 * b - a)
            x_fix[1, c, t] = -low * b
            a, b = x_high[c, t, 0], x_high[c, t, 1]
            x_fix[2, c, t] = -high * a
            x_fix[3, c, t] = high * (16.0 * a - b)

    own = count // comps
    lane8 = lane_iota(8)

    def y_rows(side, src):
        for start in range(0, own, 8):
            vals = []
            for c in range(comps):
                pair = []
                for r in range(2):
                    h = src[r, c * own + start : c * own + start + 8]
                    m2, m1, p1, p2 = (shift_lanes(h, k, lane8) for k in (-2, -1, 1, 2))
                    pair.append((h, 8.0 * (p1 - m1) - (p2 - m2)))
                (h0, d0), (h1, d1) = pair
                if side == 0:
                    vals.append(((16.0 * h1 - h0, d0 - 8.0 * d1), (-h1, d1)))
                else:
                    vals.append(((-h0, -d0), (16.0 * h0 - h1, 8.0 * d0 - d1)))
            for c in range(comps):
                for r in range(2):
                    fix = sign[c] * vals[c][r][0] - twelfth * vals[1 - c][r][1]
                    base = (side * count + c * own + start) * 8 + (0 if side == 0 else 6) + r
                    y_fix[pl.ds(base, 8, stride=8), :] = fix

    @pl.when(gy > 0)
    def _():
        y_rows(0, y_low)

    @pl.when(gy < n_y - 1)
    def _():
        y_rows(1, y_high)

    cols = count * 4 // LANES
    z_ext[...] = jnp.zeros_like(z_ext)
    spot = lane_iota(cy) % 4
    spot32 = lane_iota(cy + 16) % 4
    for col in range(cols):
        z_ext[col, 8 : 8 + cy] = jnp.where(spot < 2, z_low[col] * has_z[0], z_high[col] * has_z[1])
        z_ext[col, 6:8] = has_y[0] * jnp.where(
            spot[:2] < 2, ll[col, cy - 2 :] * has_z[0], lh[col, cy - 2 :] * has_z[1]
        )
        z_ext[col, 8 + cy : 10 + cy] = has_y[1] * jnp.where(
            spot[:2] < 2, hl[col, :2] * has_z[0], hh[col, :2] * has_z[1]
        )
    seconds = []
    for col in range(cols):
        v = z_ext[col]
        r2, l2 = pltpu.roll(v, 2, 1), pltpu.roll(v, LANES - 2, 1)
        r1, l1 = pltpu.roll(v, 1, 1), pltpu.roll(v, LANES - 1, 1)
        far = jnp.where(spot32 >= 2, r2, l2)
        near = jnp.where(spot32 == 2, r1, jnp.where(spot32 == 1, l1, 0.0))
        signed = jnp.where(spot32 >= 2, far - 8.0 * near, 8.0 * near - far)
        z_dz[col] = signed
        seconds.append((16.0 * near - far)[8 : 8 + cy])
    for col in range(cols):
        c = col // (cols // comps)
        other = col + cols // comps if c == 0 else col - cols // comps
        at = lambda k: z_dz[other, 8 + k : 8 + k + cy]
        mix = 8.0 * (at(1) - at(-1)) - (at(2) - at(-2))
        z_fix[col] = -sign[c] * seconds[col] - twelfth * mix

    lane = lane_iota(cy)
    edge = (lane < 2) | (lane >= LANES - 2)
    total_x, total_y, total_z = n_x * cx, n_y * cy, n_z * cz
    at_y = (row_iota(cy) + gy * cy).astype(F32)
    at_z = (lane + gz * cz).astype(F32)
    uy = (at_y + 0.5) / total_y - 0.5
    uz = (at_z + 0.5) / total_z - 0.5
    yz = uy * uy + uz * uz
    low_bits = low_count.bit_length() - 1
    row8 = row_iota(8)
    high_rows = [row8 + k for k in range(0, high_count, 8)]
    low_rows = [row8 + k for k in range(0, low_count, 8)]
    y_mask = ((row8 < 2) & (gy > 0), (row8 >= 6) & (gy < n_y - 1))
    per = LANES // 4

    def bin_plane(x, slot):
        outer = (x < 2) | (x >= cx - 2)
        layer = jnp.where(x < 2, x, jnp.maximum(x - (cx - 4), 0))
        for c in range(comps):
            for t in range(steps):
                k = t * cx
                col = (c * own + k) // per
                fix = pltpu.roll(z_fix[col], (LANES - 2 - 4 * (k % per + x)) % LANES, 1)
                v = local_ref[c, t, x] + jnp.where(edge, fix, 0.0)
                v = v + jnp.where(outer, x_fix[layer, c, t], 0.0)
                row = (c * own + k + x) * 8
                y_low_fix = jnp.where(y_mask[0], y_fix[pl.ds(row, 8), :], 0.0)
                y_high_fix = jnp.where(y_mask[1], y_fix[pl.ds(row + count * 8, 8), :], 0.0)
                psi_ref[c, t, x, :8] = v[:8] + y_low_fix
                if cy > 16:
                    psi_ref[c, t, x, 8 : cy - 8] = v[8 : cy - 8]
                psi_ref[c, t, x, cy - 8 :] = v[cy - 8 :] + y_high_fix

        ux = ((gx * cx + x).astype(F32) + 0.5) / total_x - 0.5
        weight = 0.0625 * (ux * ux + yz + 0.05)
        real = jnp.zeros((cy, LANES), F32)
        imag = jnp.zeros((cy, LANES), F32)
        for t in range(steps):
            real = real + psi_ref[0, t, x]
            imag = imag + psi_ref[1, t, x]
            flux = weight * (real * real + imag * imag)
            head = flux.astype(jnp.bfloat16).astype(F32)
            flux_ref[slot, 0, t] = head
            flux_ref[slot, 1, t] = flux - head
        left, right = [], []
        for y in range(cy):
            shell = jnp.broadcast_to(shell_ref[x, pl.ds(y, 1), :], (8, LANES))
            high, low = shell >> low_bits, shell & (low_count - 1)
            hot = [jnp.where(low == r, 1.0, 0.0) for r in low_rows]
            right.append(jnp.concatenate(hot).astype(jnp.bfloat16))
            masks = [high == r for r in high_rows]
            pieces = []
            for t in range(steps):
                for part in range(2):
                    f = jnp.broadcast_to(flux_ref[slot, part, t, pl.ds(y, 1), :], (8, LANES))
                    pieces.extend(jnp.where(m, f, 0.0) for m in masks)
            left.append(jnp.concatenate(pieces).astype(jnp.bfloat16))
        return lax.dot_general(
            jnp.concatenate(left, axis=1),
            jnp.concatenate(right, axis=1),
            (((1,), (1,)), ((), ())),
            preferred_element_type=F32,
        )

    def planes(i, total):
        for k in range(unroll):
            total = total + bin_plane(unroll * i + k, k)
        done = pl.ds(unroll * i, unroll)
        pltpu.make_async_copy(psi_ref.at[:, :, done], psi_out.at[:, :, done], sent).start()
        return total

    unroll = flux_ref.shape[0]
    rows = 2 * steps * high_count
    total = lax.fori_loop(0, cx // unroll, planes, jnp.zeros((rows, low_count), F32))
    scale = 0.25 * (high_count * low_count) / (total_x * total_y * total_z)
    onset = onset_ref[:, :low_count]
    running = jnp.zeros((high_count, low_count), F32)
    sums = []
    for t in range(steps):
        a = total[2 * t * high_count : (2 * t + 1) * high_count]
        b = total[(2 * t + 1) * high_count : (2 * t + 2) * high_count]
        running = running + jnp.where(t >= onset, a + b, 0.0)
        sums.append(running * scale)
    if len(part_ref.shape) == 4:
        for g in range(n_x):
            for t in range(steps):
                part_ref[g, :, t] = jnp.where(gx <= g, sums[t], 0.0)
    else:
        joined = jnp.concatenate(sums, axis=1)
        for g in range(n_x):
            part_ref[g] = jnp.where(gx <= g, joined, 0.0)
    pltpu.make_async_copy(psi_ref, psi_out, sent).wait()


def onset_table(onset_ref, high_count, low_count):
    fold = LANES // low_count
    row = row_iota(high_count)
    table = jnp.zeros((high_count, LANES), jnp.int32)
    for h in range(high_count):
        line = jnp.broadcast_to(onset_ref[h // fold : h // fold + 1], (high_count, LANES))
        line = pltpu.roll(line, (LANES - (h % fold) * low_count) % LANES, 1)
        table = jnp.where(row == h, line, table)
    return table


def sum_kernel(got_ref, out_ref):
    steps, per = out_ref.shape[1:]
    total = jnp.sum(got_ref[...], axis=0, keepdims=True)
    for t in range(steps):
        out_ref[0, t : t + 1, :] = total[:, t * per : (t + 1) * per]


def call(kernel, outs, scratch=(), flops=0, ints=0, in_hbm=0):
    place = lambda i: pl.BlockSpec(memory_space=pl.ANY if i < in_hbm else pltpu.VMEM)
    return pl.pallas_call(
        kernel,
        out_shape=tuple(
            jax.ShapeDtypeStruct(s, jnp.int32 if i < ints else F32) for i, s in enumerate(outs)
        ),
        out_specs=tuple(place(i) for i in range(len(outs))),
        scratch_shapes=scratch,
        compiler_params=pltpu.CompilerParams(vmem_limit_bytes=VMEM_LIMIT),
        cost_estimate=pl.CostEstimate(flops=flops, transcendentals=0, bytes_accessed=2**20),
    )


def ring(value, axis, shift):
    count = lax.axis_size(axis)
    return lax.ppermute(value, axis, [(i, (i + shift) % count) for i in range(count)])


def corner(value, n_y, n_z, dy, dz):
    pairs = [
        (a * n_z + b, ((a + dy) % n_y) * n_z + (b + dz) % n_z) for a in range(n_y) for b in range(n_z)
    ]
    return lax.ppermute(value, ("gy", "gz"), pairs)


def body(strain, cell_shell_index, onset_step):
    comps, steps, cx, cy, cz = strain.shape
    sizes = n_x, n_y, n_z = tuple(lax.axis_size(a) for a in ("gx", "gy", "gz"))
    shells = onset_step.shape[0]
    low_count = 32
    high_count = shells // low_count
    count = comps * steps * cx
    two_y = n_y == 2
    x_msg = (comps, steps, 2, cy, cz)
    y_msg = (2, count, cz)
    z_msg = (count * 4 // LANES, cy, LANES)
    sent = call(
        lambda *refs: pack_kernel(two_y, *refs),
        (x_msg, x_msg, z_msg) + (y_msg,) * (1 if two_y else 2),
    )(strain)
    x_tail, x_head, z_edges = sent[:3]
    x_low, x_high = ring(x_tail, "gx", 1), ring(x_head, "gx", -1)
    if two_y:
        y_low = y_high = ring(sent[3], "gy", 1)
    else:
        y_low, y_high = ring(sent[3], "gy", 1), ring(sent[4], "gy", -1)
    z_low, z_high = ring(z_edges, "gz", 1), ring(z_edges, "gz", -1)
    ll, lh = corner(z_edges, n_y, n_z, 1, 1), corner(z_edges, n_y, n_z, 1, -1)
    if two_y:
        hl, hh = ll, lh
    else:
        hl, hh = corner(z_edges, n_y, n_z, -1, 1), corner(z_edges, n_y, n_z, -1, -1)

    table, local = call(
        lambda *refs: local_kernel(low_count, *refs),
        ((high_count, LANES), strain.shape),
        [pltpu.VMEM((steps, comps, 2, cy + 16, cz), F32)],
        flops=10**8,
        ints=1,
    )(strain, onset_step.reshape(-1, LANES))

    shards = n_y * n_z
    per = shells // shards
    direct = per == low_count and steps * per == LANES
    own_rows = 2 * count * 8
    unroll = next(u for u in (UNROLL, 4, 2, 1) if cx % u == 0)
    psi, part = call(
        lambda *refs: finish_kernel(sizes, high_count, low_count, *refs),
        (strain.shape, (n_x, shards, LANES) if direct else (n_x, high_count, steps, low_count)),
        [
            pltpu.VMEM(strain.shape, F32),
            pltpu.SemaphoreType.DMA(()),
            pltpu.VMEM((4, comps, steps, cy, cz), F32),
            pltpu.VMEM((own_rows, cz), F32),
            pltpu.VMEM((z_msg[0], cy + 16, LANES), F32),
            pltpu.VMEM((z_msg[0], cy + 16, LANES), F32),
            pltpu.VMEM(z_msg, F32),
            pltpu.VMEM((unroll, 2, steps, cy, cz), F32),
        ],
        flops=10**8,
        in_hbm=1,
    )(
        local, cell_shell_index, table,
        x_low, x_high, y_low, y_high, z_low, z_high, ll, lh, hl, hh,
    )

    axes = ("gx", "gy", "gz")
    if direct:
        got = lax.all_to_all(part.reshape(n_x * shards, LANES), axes, 0, 0, tiled=True)
        return psi, call(sum_kernel, ((1, steps, per),))(got)[0]
    part = part.transpose(0, 2, 1, 3).reshape(n_x, steps, shards, per).transpose(0, 2, 1, 3)
    got = lax.all_to_all(part.reshape(n_x * shards, steps, per), axes, 0, 0, tiled=True)
    return psi, jnp.sum(got, axis=0)[None]


def solution(mesh):
    placed = (P(None, None, "gx", "gy", "gz"), P("gx", "gy", "gz"), P())
    return jax.shard_map(
        body,
        mesh=mesh,
        in_specs=placed,
        out_specs=(P(None, None, "gx", "gy", "gz"), P("gx", None, ("gy", "gz"))),
        check_vma=False,
    )
```

```python
import jax
import jax.numpy as jnp
from jax import lax
from jax.experimental import pallas as pl
from jax.experimental.pallas import tpu as pltpu
from jax.sharding import PartitionSpec as P


LANES = 128
F32 = jnp.float32
UNROLL = 16
VMEM_LIMIT = 24 * 2**20


def lane_iota(rows):
    return lax.broadcasted_iota(jnp.int32, (rows, LANES), 1)


def row_iota(rows):
    return lax.broadcasted_iota(jnp.int32, (rows, LANES), 0)


def shift_lanes(v, offset, lane):
    moved = pltpu.roll(v, (-offset) % LANES, 1)
    inside = lane < LANES - offset if offset > 0 else lane >= -offset
    return jnp.where(inside, moved, 0.0)


def pack_kernel(two_y, s_ref, *outs):
    comps, steps, cx, cy, cz = s_ref.shape
    x_near, x_far, z_edges = outs[:3]
    y_sends, corners = outs[3 : 3 + len(outs[3:]) // 2], outs[3 + len(outs[3:]) // 2 :]
    odd = lax.axis_index("gx") % 2
    near, far = (1 - odd) * (cx - 2), odd * (cx - 2)
    for c in range(comps):
        for t in range(steps):
            x_near[c, t] = s_ref[c, t, pl.ds(near, 2)]
            x_far[c, t] = s_ref[c, t, pl.ds(far, 2)]
    rows = s_ref.reshape(comps * steps * cx * cy, cz)
    count = comps * steps * cx
    if two_y:
        start = jnp.where(lax.axis_index("gy") == 0, cy - 2, 0)
        starts = (start,)
    else:
        starts = (cy - 2, 0)
    group8 = lane_iota(8) // 4
    for send, pack, start in zip(y_sends, corners, starts):
        for r in range(2):
            packed = jnp.zeros((8, LANES), F32)
            for j in range(count // 8):
                block = rows[pl.ds(start + r + 8 * j * cy, 8, stride=cy), :]
                send[r, 8 * j : 8 * j + 8] = block
                packed = jnp.where(group8 == j, pltpu.roll(block, (2 + 4 * j) % LANES, 1), packed)
            pack[8 * r : 8 * r + 8] = packed
    lane = lane_iota(cy)
    group = lane // 4
    per = LANES // 4
    for col in range(count // per):
        packed = jnp.zeros((cy, LANES), F32)
        for i in range(per):
            k = col * per + i
            block = s_ref[k // (steps * cx), (k // cx) % steps, k % cx]
            packed = jnp.where(group == i, pltpu.roll(block, (2 + 4 * i) % LANES, 1), packed)
        z_edges[col] = packed


def join_kernel(edges_ref, *refs):
    *corners, out = refs
    cols, _ = edges_ref.shape[:2]
    out[:cols] = edges_ref[...]
    for s, corner in enumerate(corners):
        out[cols + s, :16] = corner[...]


def local_kernel(low_count, s_ref, after_ref, onset_ref, table, psi_ref, pad_ref):
    table[...] = onset_table(onset_ref, table.shape[0], low_count)
    comps, steps, cx, cy, _ = s_ref.shape
    lane = lane_iota(cy)
    pad_ref[...] = jnp.zeros_like(pad_ref)

    def plane(x, carry):
        for t in range(steps):
            lap, mix = [], []
            for c in range(comps):
                s = s_ref[c, t, x]
                m2, m1, p1, p2 = (shift_lanes(s, k, lane) for k in (-2, -1, 1, 2))
                near_z, far_z = m1 + p1, m2 + p2
                first_z = 8.0 * (p1 - m1) - (p2 - m2)
                pad_ref[t, c, 0, 8 : 8 + cy] = s
                pad_ref[t, c, 1, 8 : 8 + cy] = first_z
                at = lambda q, k: pad_ref[t, c, q, 8 + k : 8 + k + cy]
                near, far = at(0, -1) + at(0, 1), at(0, -2) + at(0, 2)
                for k in (1, 2):
                    low = s_ref[c, t, jnp.maximum(x - k, 0)] * (x >= k).astype(F32)
                    high = s_ref[c, t, jnp.minimum(x + k, cx - 1)] * (x < cx - k).astype(F32)
                    if k == 1:
                        near = near + (low + high)
                    else:
                        far = far + (low + high)
                lap.append(16.0 * (near - near_z) - (far - far_z) - 30.0 * s)
                mix.append(8.0 * (at(1, 1) - at(1, -1)) - (at(1, 2) - at(1, -2)))
            psi_ref[0, t, x] = (0.5 / 12.0) * lap[0] - (1.0 / 144.0) * mix[1]
            psi_ref[1, t, x] = (-0.5 / 12.0) * lap[1] - (1.0 / 144.0) * mix[0]
        return carry

    lax.fori_loop(0, cx, plane, 0)


def finish_kernel(
    sizes, high_count, low_count,
    local_ref, shell_ref, onset_ref,
    x_near, x_far, y_low, y_high, z_low, z_high,
    psi_out, part_ref,
    psi_ref, sent, x_fix, y_fix, z_dz, z_fix, flux_ref,
):
    comps, steps, cx, cy, cz = local_ref.shape
    n_x, n_y, n_z = sizes
    gx, gy, gz = (lax.axis_index(a) for a in ("gx", "gy", "gz"))
    half, twelfth = 0.5 / 12.0, 1.0 / 144.0
    sign = (half, -half)
    has = lambda ok: ok.astype(F32)
    has_x = (has(gx > 0), has(gx < n_x - 1))
    has_y = (has(gy > 0), has(gy < n_y - 1))
    has_z = (has(gz > 0), has(gz < n_z - 1))
    count = comps * steps * cx

    odd_x = gx % 2 == 1
    for c in range(comps):
        low, high = sign[c] * has_x[0], sign[c] * has_x[1]
        for t in range(steps):
            p, q = x_near[c, t], x_far[c, t]
            below, above = jnp.where(odd_x, p, q), jnp.where(odd_x, q, p)
            a, b = below[0], below[1]
            x_fix[0, c, t] = low * (16.0 * b - a)
            x_fix[1, c, t] = -low * b
            a, b = above[0], above[1]
            x_fix[2, c, t] = -high * a
            x_fix[3, c, t] = high * (16.0 * a - b)

    own = count // comps
    lane8 = lane_iota(8)
    edge8 = (lane8 < 2) | (lane8 >= LANES - 2)
    cols = count * 4 // LANES

    def halo_terms(v, spot):
        r2, l2 = pltpu.roll(v, 2, 1), pltpu.roll(v, LANES - 2, 1)
        r1, l1 = pltpu.roll(v, 1, 1), pltpu.roll(v, LANES - 1, 1)
        far = jnp.where(spot >= 2, r2, l2)
        near = jnp.where(spot == 2, r1, jnp.where(spot == 1, l1, 0.0))
        first = jnp.where(spot >= 2, far - 8.0 * near, 8.0 * near - far)
        return first, 16.0 * near - far

    def beyond(index, rows, spot):
        low, high = z_low[index, rows] * has_z[0], z_high[index, rows] * has_z[1]
        return halo_terms(jnp.where(spot < 2, low, high), spot)

    def y_rows(side, src):
        block = cols + min(side, z_low.shape[0] - cols - 1)
        corner = [beyond(block, pl.ds(8 * r, 8), lane8 % 4)[0] for r in range(2)]
        for start in range(0, own, 8):
            vals = []
            for c in range(comps):
                pair = []
                for r in range(2):
                    h = src[r, c * own + start : c * own + start + 8]
                    m2, m1, p1, p2 = (shift_lanes(h, k, lane8) for k in (-2, -1, 1, 2))
                    k = c * own + start
                    lanes = pltpu.roll(corner[r], (LANES - 2 - k // 2) % LANES, 1)
                    first_z = 8.0 * (p1 - m1) - (p2 - m2) + jnp.where(edge8, lanes, 0.0)
                    pair.append((h, first_z))
                (h0, d0), (h1, d1) = pair
                if side == 0:
                    vals.append(((16.0 * h1 - h0, d0 - 8.0 * d1), (-h1, d1)))
                else:
                    vals.append(((-h0, -d0), (16.0 * h0 - h1, 8.0 * d0 - d1)))
            for c in range(comps):
                for r in range(2):
                    fix = sign[c] * vals[c][r][0] - twelfth * vals[1 - c][r][1]
                    base = (side * count + c * own + start) * 8 + (0 if side == 0 else 6) + r
                    y_fix[pl.ds(base, 8, stride=8), :] = fix

    @pl.when(gy > 0)
    def _():
        y_rows(0, y_low)

    @pl.when(gy < n_y - 1)
    def _():
        y_rows(1, y_high)

    spot = lane_iota(cy) % 4
    seconds = []
    for col in range(cols):
        first, second = beyond(col, pl.ds(0, cy), spot)
        z_dz[col, :8] = jnp.zeros((8, LANES), F32)
        z_dz[col, 8 : 8 + cy] = first
        z_dz[col, 8 + cy :] = jnp.zeros((8, LANES), F32)
        seconds.append(second)
    for col in range(cols):
        c = col // (cols // comps)
        other = col + cols // comps if c == 0 else col - cols // comps
        at = lambda k: z_dz[other, 8 + k : 8 + k + cy]
        mix = 8.0 * (at(1) - at(-1)) - (at(2) - at(-2))
        z_fix[col] = -sign[c] * seconds[col] - twelfth * mix

    lane = lane_iota(cy)
    edge = (lane < 2) | (lane >= LANES - 2)
    total_x, total_y, total_z = n_x * cx, n_y * cy, n_z * cz
    at_y = (row_iota(cy) + gy * cy).astype(F32)
    at_z = (lane + gz * cz).astype(F32)
    uy = (at_y + 0.5) / total_y - 0.5
    uz = (at_z + 0.5) / total_z - 0.5
    yz = uy * uy + uz * uz
    low_bits = low_count.bit_length() - 1
    row8 = row_iota(8)
    high_rows = [row8 + k for k in range(0, high_count, 8)]
    low_rows = [row8 + k for k in range(0, low_count, 8)]
    y_mask = ((row8 < 2) & (gy > 0), (row8 >= 6) & (gy < n_y - 1))
    per = LANES // 4

    def bin_plane(x, slot):
        outer = (x < 2) | (x >= cx - 2)
        layer = jnp.where(x < 2, x, jnp.maximum(x - (cx - 4), 0))
        for c in range(comps):
            for t in range(steps):
                k = t * cx
                col = (c * own + k) // per
                fix = pltpu.roll(z_fix[col], (LANES - 2 - 4 * (k % per + x)) % LANES, 1)
                v = local_ref[c, t, x] + jnp.where(edge, fix, 0.0)
                v = v + jnp.where(outer, x_fix[layer, c, t], 0.0)
                row = (c * own + k + x) * 8
                y_low_fix = jnp.where(y_mask[0], y_fix[pl.ds(row, 8), :], 0.0)
                y_high_fix = jnp.where(y_mask[1], y_fix[pl.ds(row + count * 8, 8), :], 0.0)
                psi_ref[c, t, x, :8] = v[:8] + y_low_fix
                if cy > 16:
                    psi_ref[c, t, x, 8 : cy - 8] = v[8 : cy - 8]
                psi_ref[c, t, x, cy - 8 :] = v[cy - 8 :] + y_high_fix

        ux = ((gx * cx + x).astype(F32) + 0.5) / total_x - 0.5
        weight = 0.0625 * (ux * ux + yz + 0.05)
        real = jnp.zeros((cy, LANES), F32)
        imag = jnp.zeros((cy, LANES), F32)
        for t in range(steps):
            real = real + psi_ref[0, t, x]
            imag = imag + psi_ref[1, t, x]
            flux = weight * (real * real + imag * imag)
            head = flux.astype(jnp.bfloat16).astype(F32)
            flux_ref[slot, 0, t] = head
            flux_ref[slot, 1, t] = flux - head
        left, right = [], []
        for y in range(cy):
            shell = jnp.broadcast_to(shell_ref[x, pl.ds(y, 1), :], (8, LANES))
            high, low = shell >> low_bits, shell & (low_count - 1)
            hot = [jnp.where(low == r, 1.0, 0.0) for r in low_rows]
            right.append(jnp.concatenate(hot).astype(jnp.bfloat16))
            masks = [high == r for r in high_rows]
            pieces = []
            for t in range(steps):
                for part in range(2):
                    f = jnp.broadcast_to(flux_ref[slot, part, t, pl.ds(y, 1), :], (8, LANES))
                    pieces.extend(jnp.where(m, f, 0.0) for m in masks)
            left.append(jnp.concatenate(pieces).astype(jnp.bfloat16))
        return lax.dot_general(
            jnp.concatenate(right, axis=1),
            jnp.concatenate(left, axis=1),
            (((1,), (1,)), ((), ())),
            preferred_element_type=F32,
        )

    def planes(i, total):
        for k in range(unroll):
            total = total + bin_plane(unroll * i + k, k)
        done = pl.ds(unroll * i, unroll)
        pltpu.make_async_copy(psi_ref.at[:, :, done], psi_out.at[:, :, done], sent).start()
        return total

    unroll = flux_ref.shape[0]
    rows = 2 * steps * high_count
    total = lax.fori_loop(0, cx // unroll, planes, jnp.zeros((low_count, rows), F32)).T
    scale = 0.25 * (high_count * low_count) / (total_x * total_y * total_z)
    onset = onset_ref[:, :low_count]
    running = jnp.zeros((high_count, low_count), F32)
    sums = []
    for t in range(steps):
        a = total[2 * t * high_count : (2 * t + 1) * high_count]
        b = total[(2 * t + 1) * high_count : (2 * t + 2) * high_count]
        running = running + jnp.where(t >= onset, a + b, 0.0)
        sums.append(running * scale)
    if len(part_ref.shape) == 4:
        for g in range(n_x):
            for t in range(steps):
                part_ref[g, :, t] = jnp.where(gx <= g, sums[t], 0.0)
    else:
        joined = jnp.concatenate(sums, axis=1)
        for g in range(n_x):
            part_ref[g] = jnp.where(gx <= g, joined, 0.0)
    pltpu.make_async_copy(psi_ref, psi_out, sent).wait()


def onset_table(onset_ref, high_count, low_count):
    fold = LANES // low_count
    row = row_iota(high_count)
    table = jnp.zeros((high_count, LANES), jnp.int32)
    for h in range(high_count):
        line = jnp.broadcast_to(onset_ref[h // fold : h // fold + 1], (high_count, LANES))
        line = pltpu.roll(line, (LANES - (h % fold) * low_count) % LANES, 1)
        table = jnp.where(row == h, line, table)
    return table


def sum_kernel(got_ref, out_ref):
    steps, per = out_ref.shape[1:]
    total = jnp.sum(got_ref[...], axis=0, keepdims=True)
    for t in range(steps):
        out_ref[0, t : t + 1, :] = total[:, t * per : (t + 1) * per]


def call(kernel, outs, scratch=(), flops=0, ints=0, in_hbm=0):
    place = lambda i: pl.BlockSpec(memory_space=pl.ANY if i < in_hbm else pltpu.VMEM)
    return pl.pallas_call(
        kernel,
        out_shape=tuple(
            jax.ShapeDtypeStruct(s, jnp.int32 if i < ints else F32) for i, s in enumerate(outs)
        ),
        out_specs=tuple(place(i) for i in range(len(outs))),
        scratch_shapes=scratch,
        compiler_params=pltpu.CompilerParams(vmem_limit_bytes=VMEM_LIMIT),
        cost_estimate=pl.CostEstimate(flops=flops, transcendentals=0, bytes_accessed=2**20),
    )


def ring(value, axis, shift):
    count = lax.axis_size(axis)
    return lax.ppermute(value, axis, [(i, (i + shift) % count) for i in range(count)])


def pairs(value, first):
    n_x, n_z = lax.axis_size("gx"), lax.axis_size("gz")

    def partner(x, z):
        other = x + 1 if (x - first) % 2 == 0 else x - 1
        if 0 <= other < n_x:
            return other, z
        return x, z ^ 1 if (z ^ 1) < n_z else z

    order = []
    for x in range(n_x):
        for z in range(n_z):
            p, q = partner(x, z)
            order.append((x * n_z + z, p * n_z + q))
    return lax.ppermute(value, ("gx", "gz"), order)


def body(strain, cell_shell_index, onset_step):
    comps, steps, cx, cy, cz = strain.shape
    sizes = n_x, n_y, n_z = tuple(lax.axis_size(a) for a in ("gx", "gy", "gz"))
    shells = onset_step.shape[0]
    low_count = 32
    high_count = shells // low_count
    count = comps * steps * cx
    two_y = n_y == 2
    x_msg = (comps, steps, 2, cy, cz)
    y_msg = (2, count, cz)
    z_msg = (count * 4 // LANES, cy, LANES)
    n_sides = 1 if two_y else 2
    sent = call(
        lambda *refs: pack_kernel(two_y, *refs),
        (x_msg, x_msg, z_msg) + (y_msg,) * n_sides + ((16, LANES),) * n_sides,
    )(strain)
    x_near, x_far, z_edges = sent[:3]
    sides = (1,) if two_y else (1, -1)
    corners = [ring(v, "gy", d) for v, d in zip(sent[3 + len(sides) :], sides)]
    z_edges = call(join_kernel, ((z_msg[0] + len(sides),) + z_msg[1:],))(z_edges, *corners)[0]
    halos = [ring(v, "gy", d) for v, d in zip(sent[3:], sides)]
    x_near = pairs(x_near, 0)
    x_far = pairs(x_far, 1)
    y_low, y_high = halos[0], halos[-1]
    z_low, z_high = ring(z_edges, "gz", 1), ring(z_edges, "gz", -1)
    table, local = call(
        lambda *refs: local_kernel(low_count, *refs),
        ((high_count, LANES), strain.shape),
        [pltpu.VMEM((steps, comps, 2, cy + 16, cz), F32)],
        flops=10**8,
        ints=1,
    )(strain, z_edges, onset_step.reshape(-1, LANES))

    shards = n_y * n_z
    per = shells // shards
    direct = per == low_count and steps * per == LANES
    own_rows = 2 * count * 8
    unroll = next(u for u in (UNROLL, 8, 4, 2, 1) if cx % u == 0)
    psi, part = call(
        lambda *refs: finish_kernel(sizes, high_count, low_count, *refs),
        (strain.shape, (n_x, shards, LANES) if direct else (n_x, high_count, steps, low_count)),
        [
            pltpu.VMEM(strain.shape, F32),
            pltpu.SemaphoreType.DMA(()),
            pltpu.VMEM((4, comps, steps, cy, cz), F32),
            pltpu.VMEM((own_rows, cz), F32),
            pltpu.VMEM((z_msg[0], cy + 16, LANES), F32),
            pltpu.VMEM(z_msg, F32),
            pltpu.VMEM((unroll, 2, steps, cy, cz), F32),
        ],
        flops=10**8,
        in_hbm=1,
    )(
        local, cell_shell_index, table,
        x_near, x_far, y_low, y_high, z_low, z_high,
    )

    axes = ("gx", "gy", "gz")
    if direct:
        got = lax.all_to_all(part.reshape(n_x * shards, LANES), axes, 0, 0, tiled=True)
        return psi, call(sum_kernel, ((1, steps, per),))(got)[0]
    part = part.transpose(0, 2, 1, 3).reshape(n_x, steps, shards, per).transpose(0, 2, 1, 3)
    got = lax.all_to_all(part.reshape(n_x * shards, steps, per), axes, 0, 0, tiled=True)
    return psi, jnp.sum(got, axis=0)[None]


def solution(mesh):
    placed = (P(None, None, "gx", "gy", "gz"), P("gx", "gy", "gz"), P())

    return jax.shard_map(
        body,
        mesh=mesh,
        in_specs=placed,
        out_specs=(P(None, None, "gx", "gy", "gz"), P("gx", None, ("gy", "gz"))),
        check_vma=False,
    )
```

```python
import jax
import jax.numpy as jnp
from jax import lax
from jax.experimental import pallas as pl
from jax.experimental.pallas import tpu as pltpu
from jax.sharding import PartitionSpec as P


LANES = 128
F32 = jnp.float32
UNROLL = 16
SECOND, MIXED = 0.5 / 12.0, 1.0 / 144.0
VMEM_LIMIT = 24 * 2**20


def lane_iota(rows):
    return lax.broadcasted_iota(jnp.int32, (rows, LANES), 1)


def row_iota(rows):
    return lax.broadcasted_iota(jnp.int32, (rows, LANES), 0)


def shift_lanes(v, offset, lane):
    moved = pltpu.roll(v, (-offset) % LANES, 1)
    inside = lane < LANES - offset if offset > 0 else lane >= -offset
    return jnp.where(inside, moved, 0.0)


def pack_kernel(two_y, s_ref, *outs):
    comps, steps, cx, cy, cz = s_ref.shape
    x_near, x_far, z_edges = outs[:3]
    y_sends, corners = outs[3 : 3 + len(outs[3:]) // 2], outs[3 + len(outs[3:]) // 2 :]
    odd = lax.axis_index("gx") % 2
    near, far = (1 - odd) * (cx - 2), odd * (cx - 2)
    for c in range(comps):
        for t in range(steps):
            x_near[c, t] = s_ref[c, t, pl.ds(near, 2)]
            x_far[c, t] = s_ref[c, t, pl.ds(far, 2)]
    rows = s_ref.reshape(comps * steps * cx * cy, cz)
    count = comps * steps * cx
    if two_y:
        start = jnp.where(lax.axis_index("gy") == 0, cy - 2, 0)
        starts = (start,)
    else:
        starts = (cy - 2, 0)
    for send, start in zip(y_sends, starts):
        for r in range(2):
            send[r] = rows[pl.ds(start + r, count, stride=cy), :]
    lane = lane_iota(cy)
    group = lane // 4
    per = LANES // 4
    for col in range(count // per):
        packed = jnp.zeros((cy, LANES), F32)
        for i in range(per):
            k = col * per + i
            block = s_ref[k // (steps * cx), (k // cx) % steps, k % cx]
            packed = jnp.where(group == i, pltpu.roll(block, (2 + 4 * i) % LANES, 1), packed)
        z_edges[col] = packed
        for corner, start in zip(corners, starts):
            corner[2 * col : 2 * col + 2] = z_edges[col, pl.ds(start, 2), :]


def join_kernel(n_y, edges_ref, low_ref, high_ref, tail, head):
    cols, cy = edges_ref.shape[:2]
    gy = lax.axis_index("gy")
    low, high = (gy > 0).astype(F32), (gy < n_y - 1).astype(F32)

    def put(at, rows, get):
        left = lane_iota(rows) % 4 < 2
        for k in range(cols // 2):
            a, b = get(2 * k), get(2 * k + 1)
            tail[k, at : at + rows] = jnp.where(left, a, pltpu.roll(b, 2, 1))
            head[k, at : at + rows] = jnp.where(left, pltpu.roll(a, LANES - 2, 1), b)

    put(0, cy, lambda col: edges_ref[col])
    put(cy, 2, lambda col: low_ref[2 * col : 2 * col + 2] * low)
    put(cy + 2, 2, lambda col: high_ref[2 * col : 2 * col + 2] * high)


def local_kernel(
    low_count, s_ref, after_ref, shell_ref, onset_ref,
    table, shell_out, psi_ref,
    pad_ref, onset_vmem, shell_sent, onset_sent,
):
    shell_load = pltpu.make_async_copy(shell_ref, shell_out, shell_sent)
    onset_load = pltpu.make_async_copy(onset_ref, onset_vmem, onset_sent)
    onset_load.start()
    shell_load.start()
    comps, steps, cx, cy, _ = s_ref.shape
    lane = lane_iota(cy)
    pad_ref[...] = jnp.zeros_like(pad_ref)

    def plane(x, slot):
        for t in range(steps):
            lap, mix = [], []
            for c in range(comps):
                s = s_ref[c, t, x]
                m2, m1, p1, p2 = (shift_lanes(s, k, lane) for k in (-2, -1, 1, 2))
                near_z, far_z = m1 + p1, m2 + p2
                first_z = 8.0 * (p1 - m1) - (p2 - m2)
                pad_ref[slot, t, c, 0, 8 : 8 + cy] = s
                pad_ref[slot, t, c, 1, 8 : 8 + cy] = first_z
                at = lambda q, k: pad_ref[slot, t, c, q, 8 + k : 8 + k + cy]
                near, far = at(0, -1) + at(0, 1), at(0, -2) + at(0, 2)
                for k in (1, 2):
                    low = s_ref[c, t, jnp.maximum(x - k, 0)] * (x >= k).astype(F32)
                    high = s_ref[c, t, jnp.minimum(x + k, cx - 1)] * (x < cx - k).astype(F32)
                    if k == 1:
                        near = near + (low + high)
                    else:
                        far = far + (low + high)
                lap.append(16.0 * (near - near_z) - (far - far_z) - 30.0 * s)
                mix.append(8.0 * (at(1, 1) - at(1, -1)) - (at(1, 2) - at(1, -2)))
            psi_ref[0, t, x] = (0.5 / 12.0) * lap[0] - (1.0 / 144.0) * mix[1]
            psi_ref[1, t, x] = (-0.5 / 12.0) * lap[1] - (1.0 / 144.0) * mix[0]

    group = pad_ref.shape[0]

    def planes(i, carry):
        for k in range(group):
            plane(group * i + k, k)
        return carry

    lax.fori_loop(0, cx // group, planes, 0)
    onset_load.wait()
    table[...] = onset_table(onset_vmem, table.shape[0], low_count)
    shell_load.wait()


def faces_kernel(n_x, n_y, x_near, x_far, y_low, y_high, before_ref, psi_ref):
    comps, steps, cx, cy, cz = psi_ref.shape
    gx, gy = lax.axis_index("gx"), lax.axis_index("gy")
    sign = (SECOND, -SECOND)
    odd = gx % 2 == 1
    for c in range(comps):
        low, high = sign[c] * (gx > 0).astype(F32), sign[c] * (gx < n_x - 1).astype(F32)
        for t in range(steps):
            p, q = x_near[c, t], x_far[c, t]
            below, above = jnp.where(odd, p, q), jnp.where(odd, q, p)
            psi_ref[c, t, 0] += low * (16.0 * below[1] - below[0])
            psi_ref[c, t, 1] -= low * below[1]
            psi_ref[c, t, cx - 2] -= high * above[0]
            psi_ref[c, t, cx - 1] += high * (16.0 * above[0] - above[1])
    own = steps * cx
    rows = psi_ref.reshape(comps * own * cy, cz)
    lane8 = lane_iota(8)

    def y_rows(side, src):
        for start in range(0, own, 8):
            vals = []
            for c in range(comps):
                pair = []
                for r in range(2):
                    h = src[r, c * own + start : c * own + start + 8]
                    m2, m1, p1, p2 = (shift_lanes(h, k, lane8) for k in (-2, -1, 1, 2))
                    pair.append((h, 8.0 * (p1 - m1) - (p2 - m2)))
                (h0, d0), (h1, d1) = pair
                if side == 0:
                    vals.append(((16.0 * h1 - h0, d0 - 8.0 * d1), (-h1, d1)))
                else:
                    vals.append(((-h0, -d0), (16.0 * h0 - h1, 8.0 * d0 - d1)))
            for c in range(comps):
                for r in range(2):
                    fix = sign[c] * vals[c][r][0] - MIXED * vals[1 - c][r][1]
                    base = (c * own + start) * cy + (0 if side == 0 else cy - 2) + r
                    rows[pl.ds(base, 8, stride=cy), :] += fix

    @pl.when(gy > 0)
    def _():
        y_rows(0, y_low)

    @pl.when(gy < n_y - 1)
    def _():
        y_rows(1, y_high)


def finish_kernel(
    sizes, high_count, low_count,
    local_ref, shell_ref, onset_ref,
    z_low, z_high,
    psi_out, part_ref,
    psi_ref, sent, z_dz, z_fix, flux_ref,
):
    comps, steps, cx, cy, cz = local_ref.shape
    n_x, n_y, n_z = sizes
    gx, gy, gz = (lax.axis_index(a) for a in ("gx", "gy", "gz"))
    sign = (SECOND, -SECOND)
    has = lambda ok: ok.astype(F32)
    has_z = (has(gz > 0), has(gz < n_z - 1))
    count = comps * steps * cx

    own = count // comps
    cols = count * 4 // LANES

    def halo_terms(v, spot):
        r2, l2 = pltpu.roll(v, 2, 1), pltpu.roll(v, LANES - 2, 1)
        r1, l1 = pltpu.roll(v, 1, 1), pltpu.roll(v, LANES - 1, 1)
        far = jnp.where(spot >= 2, r2, l2)
        near = jnp.where(spot == 2, r1, jnp.where(spot == 1, l1, 0.0))
        first = jnp.where(spot >= 2, far - 8.0 * near, 8.0 * near - far)
        return first, 16.0 * near - far

    spot = lane_iota(cy + 16) % 4
    seconds = []
    z_dz[...] = jnp.zeros_like(z_dz)
    for col in range(cols):
        for place, at, rows in ((8, 0, cy), (6, cy, 2), (8 + cy, cy + 2, 2)):
            low, high = z_low[col // 2, at : at + rows], z_high[col // 2, at : at + rows]
            if col % 2:
                low = pltpu.roll(low, LANES - 2, 1)
            else:
                high = pltpu.roll(high, 2, 1)
            z_dz[col, place : place + rows] = jnp.where(spot[:rows] < 2, low * has_z[0], high * has_z[1])
        first, second = halo_terms(z_dz[col], spot)
        z_dz[col] = first
        seconds.append(second[8 : 8 + cy])
    for col in range(cols):
        c = col // (cols // comps)
        other = col + cols // comps if c == 0 else col - cols // comps
        at = lambda k: z_dz[other, 8 + k : 8 + k + cy]
        mix = 8.0 * (at(1) - at(-1)) - (at(2) - at(-2))
        z_fix[col] = -sign[c] * seconds[col] - MIXED * mix

    lane = lane_iota(cy)
    edge = (lane < 2) | (lane >= LANES - 2)
    total_x, total_y, total_z = n_x * cx, n_y * cy, n_z * cz
    at_y = (row_iota(cy) + gy * cy).astype(F32)
    at_z = (lane + gz * cz).astype(F32)
    uy = (at_y + 0.5) / total_y - 0.5
    uz = (at_z + 0.5) / total_z - 0.5
    yz = uy * uy + uz * uz
    low_bits = low_count.bit_length() - 1
    row8 = row_iota(8)
    high_rows = [row8 + k for k in range(0, high_count, 8)]
    low_rows = [row8 + k for k in range(0, low_count, 8)]
    per = LANES // 4

    def bin_plane(x, slot):
        for c in range(comps):
            for t in range(steps):
                k = t * cx
                col = (c * own + k) // per
                fix = pltpu.roll(z_fix[col], (LANES - 2 - 4 * (k % per + x)) % LANES, 1)
                psi_ref[c, t, x] = local_ref[c, t, x] + jnp.where(edge, fix, 0.0)

        ux = ((gx * cx + x).astype(F32) + 0.5) / total_x - 0.5
        weight = 0.0625 * (ux * ux + yz + 0.05)
        real = jnp.zeros((cy, LANES), F32)
        imag = jnp.zeros((cy, LANES), F32)
        for t in range(steps):
            real = real + psi_ref[0, t, x]
            imag = imag + psi_ref[1, t, x]
            flux = weight * (real * real + imag * imag)
            head = flux.astype(jnp.bfloat16).astype(F32)
            flux_ref[slot, 0, t] = head
            flux_ref[slot, 1, t] = flux - head
        left, right = [], []
        for y in range(cy):
            shell = jnp.broadcast_to(shell_ref[x, pl.ds(y, 1), :], (8, LANES))
            high, low = shell >> low_bits, shell & (low_count - 1)
            hot = [jnp.where(low == r, 1.0, 0.0) for r in low_rows]
            right.append(jnp.concatenate(hot).astype(jnp.bfloat16))
            masks = [high == r for r in high_rows]
            pieces = []
            for t in range(steps):
                for part in range(2):
                    f = jnp.broadcast_to(flux_ref[slot, part, t, pl.ds(y, 1), :], (8, LANES))
                    pieces.extend(jnp.where(m, f, 0.0) for m in masks)
            left.append(jnp.concatenate(pieces).astype(jnp.bfloat16))
        return lax.dot_general(
            jnp.concatenate(right, axis=1),
            jnp.concatenate(left, axis=1),
            (((1,), (1,)), ((), ())),
            preferred_element_type=F32,
        )

    def planes(i, total):
        for k in range(unroll):
            total = total + bin_plane(unroll * i + k, k)
            if (k + 1) % batch == 0:
                done = pl.ds(unroll * i + k + 1 - batch, batch)
                pltpu.make_async_copy(psi_ref.at[:, :, done], psi_out.at[:, :, done], sent).start()
        return total

    unroll = flux_ref.shape[0]
    batch = 4 if unroll % 4 == 0 else 1
    rows = 2 * steps * high_count
    total = lax.fori_loop(0, cx // unroll, planes, jnp.zeros((low_count, rows), F32)).T
    scale = 0.25 * (high_count * low_count) / (total_x * total_y * total_z)
    onset = onset_ref[:, :low_count]
    running = jnp.zeros((high_count, low_count), F32)
    sums = []
    for t in range(steps):
        a = total[2 * t * high_count : (2 * t + 1) * high_count]
        b = total[(2 * t + 1) * high_count : (2 * t + 2) * high_count]
        running = running + jnp.where(t >= onset, a + b, 0.0)
        sums.append(running * scale)
    if len(part_ref.shape) == 4:
        for g in range(n_x):
            for t in range(steps):
                part_ref[g, :, t] = jnp.where(gx <= g, sums[t], 0.0)
    else:
        joined = jnp.concatenate(sums, axis=1)
        for g in range(n_x):
            part_ref[g] = jnp.where(gx <= g, joined, 0.0)
    pltpu.make_async_copy(psi_ref, psi_out, sent).wait()


def onset_table(onset_ref, high_count, low_count):
    fold = LANES // low_count
    row = row_iota(high_count)
    table = jnp.zeros((high_count, LANES), jnp.int32)
    for h in range(high_count):
        line = jnp.broadcast_to(onset_ref[h // fold : h // fold + 1], (high_count, LANES))
        line = pltpu.roll(line, (LANES - (h % fold) * low_count) % LANES, 1)
        table = jnp.where(row == h, line, table)
    return table


def sum_kernel(got_ref, out_ref):
    steps, per = out_ref.shape[1:]
    total = jnp.sum(got_ref[...], axis=0, keepdims=True)
    for t in range(steps):
        out_ref[0, t : t + 1, :] = total[:, t * per : (t + 1) * per]


def call(kernel, outs, scratch=(), flops=0, ints=0, in_hbm=0, aliases={}, places=()):
    place = lambda i: pl.BlockSpec(memory_space=pl.ANY if i < in_hbm else pltpu.VMEM)
    return pl.pallas_call(
        kernel,
        out_shape=tuple(
            jax.ShapeDtypeStruct(s, jnp.int32 if i < ints else F32) for i, s in enumerate(outs)
        ),
        out_specs=tuple(place(i) for i in range(len(outs))),
        scratch_shapes=scratch,
        input_output_aliases=aliases,
        **({"in_specs": [pl.BlockSpec(memory_space=p) for p in places]} if places else {}),
        compiler_params=pltpu.CompilerParams(vmem_limit_bytes=VMEM_LIMIT),
        cost_estimate=pl.CostEstimate(flops=flops, transcendentals=0, bytes_accessed=2**20),
    )


def ring(value, axis, shift):
    count = lax.axis_size(axis)
    return lax.ppermute(value, axis, [(i, (i + shift) % count) for i in range(count)])


def pairs(value, first):
    n_x, n_z = lax.axis_size("gx"), lax.axis_size("gz")

    def partner(x, z):
        other = x + 1 if (x - first) % 2 == 0 else x - 1
        if 0 <= other < n_x:
            return other, z
        return x, z ^ 1 if (z ^ 1) < n_z else z

    order = []
    for x in range(n_x):
        for z in range(n_z):
            p, q = partner(x, z)
            order.append((x * n_z + z, p * n_z + q))
    return lax.ppermute(value, ("gx", "gz"), order)


def body(strain, cell_shell_index, onset_step):
    comps, steps, cx, cy, cz = strain.shape
    sizes = n_x, n_y, n_z = tuple(lax.axis_size(a) for a in ("gx", "gy", "gz"))
    shells = onset_step.shape[0]
    low_count = 32
    high_count = shells // low_count
    count = comps * steps * cx
    two_y = n_y == 2
    x_msg = (comps, steps, 2, cy, cz)
    y_msg = (2, count, cz)
    z_msg = (count * 4 // LANES, cy, LANES)
    n_sides = 1 if two_y else 2
    sent = call(
        lambda *refs: pack_kernel(two_y, *refs),
        (x_msg, x_msg, z_msg) + (y_msg,) * n_sides + ((2 * z_msg[0], LANES),) * n_sides,
    )(strain)
    x_near, x_far, z_edges = sent[:3]
    sides = (1,) if two_y else (1, -1)
    corners = [ring(v, "gy", d) for v, d in zip(sent[3 + len(sides) :], sides)]
    tail, head = call(lambda *refs: join_kernel(n_y, *refs), ((z_msg[0] // 2, cy + 8, LANES),) * 2)(
        z_edges, corners[0], corners[-1]
    )
    halos = [ring(v, "gy", d) for v, d in zip(sent[3:], sides)]
    x_near = pairs(x_near, 0)
    x_far = pairs(x_far, 1)
    y_low, y_high = halos[0], halos[-1]
    z_low = ring(tail, "gz", 1)
    z_high = ring(head, "gz", -1)
    onset = onset_step.reshape(-1, LANES)
    held = lambda v: pltpu.with_memory_space_constraint(v, pltpu.HBM)
    table, shell_index, local = call(
        lambda *refs: local_kernel(low_count, *refs),
        ((high_count, LANES), cell_shell_index.shape, strain.shape),
        [
            pltpu.VMEM((4 if cx % 4 == 0 else 1, steps, comps, 2, cy + 16, cz), F32),
            pltpu.VMEM(onset.shape, jnp.int32),
            pltpu.SemaphoreType.DMA(()),
            pltpu.SemaphoreType.DMA(()),
        ],
        flops=10**8,
        ints=2,
        places=(pltpu.VMEM, pltpu.VMEM, pltpu.HBM, pltpu.HBM),
    )(strain, tail, held(cell_shell_index), held(onset))

    local = call(
        lambda *refs: faces_kernel(n_x, n_y, *refs), (strain.shape,), flops=10**8, aliases={4: 0}
    )(x_near, x_far, y_low, y_high, local)[0]

    shards = n_y * n_z
    per = shells // shards
    direct = per == low_count and steps * per == LANES
    unroll = next(u for u in (UNROLL, 8, 4, 2, 1) if cx % u == 0)
    psi, part = call(
        lambda *refs: finish_kernel(sizes, high_count, low_count, *refs),
        (strain.shape, (n_x, shards, LANES) if direct else (n_x, high_count, steps, low_count)),
        [
            pltpu.VMEM(strain.shape, F32),
            pltpu.SemaphoreType.DMA(()),
            pltpu.VMEM((z_msg[0], cy + 16, LANES), F32),
            pltpu.VMEM(z_msg, F32),
            pltpu.VMEM((unroll, 2, steps, cy, cz), F32),
        ],
        flops=10**8,
        in_hbm=1,
    )(
        local, shell_index, table,
        z_low, z_high,
    )

    axes = ("gx", "gy", "gz")
    if direct:
        got = lax.all_to_all(part.reshape(n_x * shards, LANES), axes, 0, 0, tiled=True)
        return psi, call(sum_kernel, ((1, steps, per),))(got)[0]
    part = part.transpose(0, 2, 1, 3).reshape(n_x, steps, shards, per).transpose(0, 2, 1, 3)
    got = lax.all_to_all(part.reshape(n_x * shards, steps, per), axes, 0, 0, tiled=True)
    return psi, jnp.sum(got, axis=0)[None]


def solution(mesh):
    placed = (P(None, None, "gx", "gy", "gz"), P("gx", "gy", "gz"), P())

    return jax.shard_map(
        body,
        mesh=mesh,
        in_specs=placed,
        out_specs=(P(None, None, "gx", "gy", "gz"), P("gx", None, ("gy", "gz"))),
        check_vma=False,
    )
```
